32 devices in a mesh: parts: 2 (over x), seq: 16 (over z, y, core).
Axes of the slice: x: 2, y: 2, z: 4, core: 2. Of those that a mesh axis runs over, the one named last changes fastest.
Arguments:
- token_ids: int32 [4, 4], P(None, 'parts'), parts along dimension 1, may hold values from 0 to 76031
- lengths: int32 [4], P('parts'), parts along dimension 0, may hold values from 24576 to 32768, as said below
- embed_table: bfloat16 [76032, 5120], P('seq'), may hold values from -6 to 6
- attn_gain: bfloat16 [5120], replicated, may hold values from 0.25 to 1.75
- w_qkv: bfloat16 [5120, 7168], P('seq'), may hold values from -0.125 to 0.125
- qkv_bias: float32 [7168], replicated, may hold values from -8 to 8
- cache_keys: bfloat16 [4, 32768, 1024], P('parts', 'seq'), parts along dimension 0, may hold values from -300 to 300
- cache_values: bfloat16 [4, 32768, 1024], P('parts', 'seq'), parts along dimension 0, may hold values from -6 to 6
- w_out: bfloat16 [5120, 5120], P(None, 'seq'), may hold values from -0.078125 to 0.078125
- mlp_gain: bfloat16 [5120], replicated, may hold values from 0.25 to 1.75
- w_gate: bfloat16 [5120, 16384], P(None, 'seq'), may hold values from -0.078125 to 0.078125
- w_up: bfloat16 [5120, 16384], P(None, 'seq'), may hold values from -0.078125 to 0.078125
- w_down: bfloat16 [16384, 5120], P('seq'), may hold values from -0.0625 to 0.0625
Outputs:
- attended: bfloat16 [4, 4, 5120], P(None, 'parts'), parts along dimension 1
- layer_out: bfloat16 [4, 4, 5120], P(None, 'parts', 'seq'), parts along dimension 1
The draws below stay inside these ranges and needn't reach their ends.
There are 2 independent parts, one for each index of `parts`. The reference program is written for one: setup_inputs(seed, part) draws one part's arguments, and reference() takes and returns one part's arrays. A program takes and returns all parts, laid end to end along the dimension named above; an argument that names none is the same for every part. Nothing has to cross between parts.
Inputs may be any that keep to these rules, and one draw needn't show every extreme that they name: Cache positions lengths[b] and later are unused; the first prompt fills the whole cache of 32768 positions.
All inputs are finite; a program needn't handle non-finite values.
Results may differ from the reference program's by a relative error of at most 0.017.
The reference program's roundings to bfloat16 on the way (of `normed`, `joint`, `normed_mid` and `hidden`) count: a program that leaves them out, or rounds other values in their place, can miss the bound.
Values may be sent and summed in bfloat16 or wider, within the bound.
A program may use at most 192 MiB of HBM per device.

```python
import jax
import jax.numpy as jnp
from jax import lax

D = 5120
HEADS = 40
KV_HEADS = 8
HEAD_DIM = 128
FF = 16384
VOCAB = 76032
CTX = 32768
STEPS = 4
SEQS = 2
QD = 5120
KVD = 1024
QKV = 7168


def draw_lengths(key, part):
    drawn = jax.random.randint(jax.random.fold_in(key, 3), (SEQS,), CTX - CTX // 4, CTX + 1, dtype=jnp.int32)
    return drawn.at[0].set(CTX)


def draw_qkv_bias(key, part):
    key_one, key_two, key_three, key_four = jax.random.split(jax.random.fold_in(key, 11), 4)
    direction = jax.random.normal(key_one, (KV_HEADS, HEAD_DIM), jnp.float32)
    strength = jax.random.uniform(key_two, (KV_HEADS, 1), jnp.float32, 1.05, 1.3)
    aligned = direction * strength
    query_noise = 0.5 * jax.random.normal(key_three, (KV_HEADS, HEADS // KV_HEADS, HEAD_DIM), jnp.float32)
    query_part = (aligned[:, None, :] + query_noise).reshape(HEADS * HEAD_DIM)
    key_part = aligned.reshape(KV_HEADS * HEAD_DIM)
    value_part = 0.5 * jax.random.normal(key_four, (KV_HEADS * HEAD_DIM,), jnp.float32)
    joined = jnp.concatenate([query_part, key_part, value_part])
    return jnp.clip(joined, -8.0, 8.0)


def draw_cache_keys(key, part):
    key_one = jax.random.fold_in(jax.random.fold_in(key, 17), 0)
    base = 2.2 * jax.random.normal(key_one, (SEQS, CTX, KV_HEADS, HEAD_DIM), jnp.float32)
    return jnp.clip(base, -300.0, 300.0).reshape(SEQS, CTX, KV_HEADS * HEAD_DIM).astype(jnp.bfloat16)


def touch_ends(entries, key, low, largest):
    dims = entries.shape
    index_at = [jax.random.randint(jax.random.fold_in(key, axis), (), 0, dims[axis]) for axis in range(len(dims))]
    entries = entries.at[tuple(index_at)].set(low)
    longest = dims.index(max(dims))
    index_at[longest] = (index_at[longest] + 1) % dims[longest]
    return entries.at[tuple(index_at)].set(largest)


def spiked(values, rng, source, target, parts, factor):
    def block_of(dim):
        return (jnp.arange(values.shape[dim]) // (values.shape[dim] // parts)).reshape((-1,) + (1,) * (values.ndim - 1 - dim))

    first = jax.random.permutation(rng, parts)[block_of(target)]
    far = (block_of(target) + parts // 2) % parts
    return jnp.where((block_of(source) == first) | (block_of(source) == far), factor * values, values)


def level_of(rng, shape, shards, smallest, top_value):
    level, own = 1.0, jax.random.fold_in(rng, 6)
    for dim, parts in shards:
        steps = jnp.exp(jax.random.uniform(jax.random.fold_in(own, dim), (parts,), jnp.float32, smallest / len(shards), top_value / len(shards)))
        level = level * jnp.repeat(steps, shape[dim] // parts).reshape([-1 if axis == dim else 1 for axis in range(len(shape))])
    return level


def gaussian(key, shape, spread, most, pieces=(), held_as=jnp.bfloat16):
    values = jax.random.normal(key, shape, jnp.float32) * spread
    if len(pieces) > 0:
        values = level_of(key, shape, pieces, -0.22, 0.18) * values
    return jnp.clip(values, min=-most, max=most).astype(held_as)


def heavy_noise(own_key, shape, spread, most, shards, heavy, held_as=jnp.bfloat16):
    entries = spread * jax.random.normal(own_key, shape, jnp.float32)
    if shards:
        entries = entries * level_of(own_key, shape, shards, -0.22, 0.18)
    return jnp.clip(spiked(entries, jax.random.fold_in(own_key, 3), *heavy), -most, most).astype(held_as)


def setup_inputs(seed: int = 0, part: int = 0) -> dict:
    streams_of = jax.random.split(jax.random.key(seed), 14)
    part_keys = jax.random.split(jax.random.fold_in(streams_of[13], part), 14)
    token_ids = touch_ends(jax.random.randint(part_keys[0], (STEPS, SEQS), 0, VOCAB), jax.random.fold_in(part_keys[0], 1), 0, VOCAB - 1).astype(jnp.int32)
    lengths = draw_lengths(jax.random.fold_in(jax.random.fold_in(streams_of[13], part), 71), part)
    embed_table = gaussian(streams_of[2], (VOCAB, D), 0.5, 6.0, ((0, 16),))
    attn_gain = jnp.clip(1.0 + 0.15 * jax.random.normal(streams_of[3], (D,), jnp.float32), 0.25, 1.75).astype(jnp.bfloat16)
    w_qkv = heavy_noise(streams_of[4], (D, QKV), D ** -0.5, 0.125, ((0, 16),), (0, 1, 16, 2.0))
    qkv_bias = draw_qkv_bias(jax.random.fold_in(streams_of[13], 71), part)
    cache_keys = draw_cache_keys(jax.random.fold_in(jax.random.fold_in(streams_of[13], part), 71), part)
    cache_values = gaussian(part_keys[7], (SEQS, CTX, KVD), 1.0, 6.0, ((1, 16),))
    w_out = gaussian(streams_of[8], (QD, D), QD ** -0.5, 0.078125, ((1, 16),))
    mlp_gain = jnp.clip(1.0 + 0.15 * jax.random.normal(streams_of[9], (D,), jnp.float32), 0.25, 1.75).astype(jnp.bfloat16)
    w_gate = gaussian(streams_of[10], (D, FF), D ** -0.5, 0.078125, ((1, 16),))
    w_up = gaussian(streams_of[11], (D, FF), D ** -0.5, 0.078125, ((1, 16),))
    w_down = heavy_noise(streams_of[12], (FF, D), FF ** -0.5, 0.0625, ((0, 16),), (0, 1, 16, 2.0))
    return {"token_ids": token_ids, "lengths": lengths, "embed_table": embed_table, "attn_gain": attn_gain, "w_qkv": w_qkv, "qkv_bias": qkv_bias, "cache_keys": cache_keys, "cache_values": cache_values, "w_out": w_out, "mlp_gain": mlp_gain, "w_gate": w_gate, "w_up": w_up, "w_down": w_down}


NORM_EPS = 1e-06
ROPE_BASE = 1000000.0
MASKED = -1e+30

def rms_normalize(rows, gain):
    mean_square = lax.optimization_barrier(jnp.mean(rows * rows, axis=-1, keepdims=True))
    return (rows * lax.rsqrt(mean_square + NORM_EPS) * gain.astype(jnp.float32)).astype(jnp.bfloat16)

def rotate(vectors, positions):
    half_dim = vectors.shape[-1] // 2
    frequency = ROPE_BASE ** (-2.0 * jnp.arange(half_dim, dtype=jnp.float32) / vectors.shape[-1])
    angles = positions.astype(jnp.float32)[..., None, None] * frequency
    cosine = jnp.cos(angles)
    sine_part = jnp.sin(angles)
    widened = vectors.astype(jnp.float32)
    first_half = widened[..., :half_dim]
    second = widened[..., half_dim:]
    joined = jnp.concatenate([first_half * cosine - second * sine_part, second * cosine + first_half * sine_part], axis=-1)
    return joined.astype(jnp.bfloat16)

def attend_one(query_rows, key_rows, value_rows, cached_keys, cached_values, length):
    all_keys = jnp.concatenate([cached_keys.reshape(CTX, KV_HEADS, HEAD_DIM), key_rows], axis=0).astype(jnp.float32)
    all_values = jnp.concatenate([cached_values.reshape(CTX, KV_HEADS, HEAD_DIM), value_rows], axis=0).astype(jnp.float32)
    grouped = query_rows.reshape(STEPS, KV_HEADS, HEADS // KV_HEADS, HEAD_DIM).astype(jnp.float32)
    scores = jnp.einsum('skgd,pkd->kgsp', grouped, all_keys) * HEAD_DIM ** (-0.5)
    places = jnp.arange(CTX + STEPS, dtype=jnp.int32)
    step_index = jnp.arange(STEPS, dtype=jnp.int32)
    cache_valid = places[None, :] < length
    new_valid = places[None, :] - CTX <= step_index[:, None]
    valid = jnp.where(places[None, :] < CTX, cache_valid, new_valid)
    masked = jnp.where(valid, scores, MASKED)
    top_score = lax.optimization_barrier(jnp.max(masked, axis=-1, keepdims=True))
    weights = jnp.where(valid, jnp.exp(masked - top_score), 0.0)
    total = lax.optimization_barrier(jnp.sum(weights, axis=-1))
    rounded = lax.optimization_barrier(weights.astype(jnp.bfloat16)).astype(jnp.float32)
    summed = jnp.einsum('kgsp,pkd->kgsd', rounded, all_values)
    result = summed / total[..., None]
    result = jnp.transpose(result, (2, 0, 1, 3))
    return result.reshape(STEPS, HEADS * HEAD_DIM).astype(jnp.bfloat16)

def reference(token_ids, lengths, embed_table, attn_gain, w_qkv, qkv_bias, cache_keys, cache_values, w_out, mlp_gain, w_gate, w_up, w_down):
    query_width = HEADS * HEAD_DIM
    key_width = KV_HEADS * HEAD_DIM
    stream = embed_table[token_ids].astype(jnp.float32)
    normed = rms_normalize(stream, attn_gain)
    joint = jnp.dot(normed.reshape(-1, D), w_qkv, preferred_element_type=jnp.float32) + qkv_bias.astype(jnp.float32)
    joint = joint.astype(jnp.bfloat16).reshape(STEPS, SEQS, -1)
    query_part = joint[..., :query_width].reshape(STEPS, SEQS, HEADS, HEAD_DIM)
    key_part = joint[..., query_width:query_width + key_width].reshape(STEPS, SEQS, KV_HEADS, HEAD_DIM)
    value_part = joint[..., query_width + key_width:].reshape(STEPS, SEQS, KV_HEADS, HEAD_DIM)
    positions = lengths[None, :] + jnp.arange(STEPS, dtype=jnp.int32)[:, None]
    queries = rotate(query_part, positions)
    new_keys = rotate(key_part, positions)
    outputs = []
    for seq_index in range(SEQS):
        outputs.append(attend_one(queries[:, seq_index], new_keys[:, seq_index], value_part[:, seq_index], cache_keys[seq_index], cache_values[seq_index], lengths[seq_index]))
    attended = jnp.stack(outputs, axis=1)
    projected = jnp.dot(attended.reshape(-1, query_width), w_out, preferred_element_type=jnp.float32)
    mid = stream + projected.reshape(STEPS, SEQS, D)
    normed_mid = rms_normalize(mid, mlp_gain).reshape(-1, D)
    gate = jnp.dot(normed_mid, w_gate, preferred_element_type=jnp.float32)
    upper = jnp.dot(normed_mid, w_up, preferred_element_type=jnp.float32)
    hidden = (jax.nn.silu(gate) * upper).astype(jnp.bfloat16)
    down = jnp.dot(hidden, w_down, preferred_element_type=jnp.float32).reshape(STEPS, SEQS, D)
    layer_out = (mid + down).astype(jnp.bfloat16)
    return (attended, layer_out)
```

```python
import functools
import math

import jax
import jax.numpy as jnp
import numpy as np
from jax import lax
from jax.experimental import pallas as pl
from jax.experimental.pallas import tpu as pltpu
from jax.sharding import PartitionSpec as P

HEADS = 40
KV_HEADS = 8
HEAD_DIM = 128
GROUP = HEADS // KV_HEADS
LOCAL = GROUP + 2
LANES = 128

NORM_EPS = 1e-06
ROPE_BASE = 1000000.0
MASKED = -1e30
F32 = jnp.float32
BF16 = jnp.bfloat16
MESH = pl.DeviceIdType.MESH

FIRST_RECEIVE = (0, 1, 2, 2 + KV_HEADS, 3 + KV_HEADS, 3 + 2 * KV_HEADS, 11 + 2 * KV_HEADS)
RECEIVES = 12 + 2 * KV_HEADS


def pieces_of(value, count):
    out = []
    for _ in range(count):
        piece = value.astype(BF16).astype(F32)
        out.append(piece)
        value = value - piece
    return out


def gather_kernel(
    n,
    ids_hbm,
    lengths_hbm,
    gain_one_hbm,
    gain_two_hbm,
    table,
    blocks,
    gains,
    misc,
    ids,
    lengths,
    gain_one,
    gain_two,
    rows,
    wide,
    sem,
    row_sem,
):
    me = lax.axis_index("seq")
    small = [
        pltpu.make_async_copy(a, b, sem.at[i])
        for i, (a, b) in enumerate(
            (
                (ids_hbm, ids),
                (lengths_hbm, lengths),
                (gain_one_hbm, gain_one),
                (gain_two_hbm, gain_two),
            )
        )
    ]
    for copy in small:
        copy.start()
    first = lax.broadcasted_iota(jnp.int32, (1, LANES), 1)
    half = HEAD_DIM // 2
    frequency = jnp.zeros((1, LANES), F32)
    for i in range(half):
        value = float(np.float32(ROPE_BASE ** (-2.0 * i / HEAD_DIM)))
        frequency = jnp.where(first % half == i, value, frequency)
    batches, steps = ids.shape
    small[0].wait()
    tokens = batches * steps
    vocab_rows, width = table.shape
    cols = width // n
    row = lax.broadcasted_iota(jnp.int32, (tokens, tokens * 8), 0)
    lane = lax.broadcasted_iota(jnp.int32, (tokens, tokens * 8), 1)
    target = jnp.full((tokens, tokens * 8), -1, jnp.int32)
    copies = []
    for t in range(tokens):
        local = ids[t // steps, t % steps] - me * vocab_rows
        inside = (local >= 0) & (local < vocab_rows)
        local = jnp.clip(local, 0, vocab_rows - 1)
        base = local // 8
        copy = pltpu.make_async_copy(
            table.at[pl.ds(pl.multiple_of(base * 8, 8), 8), :], rows.at[t], row_sem.at[t]
        )
        copy.start()
        copies.append(copy)
        target = jnp.where(row == t, jnp.where(inside, t * 8 + local - base * 8, -1), target)
    one_hot = jnp.where(lane == target, 1.0, 0.0).astype(BF16)

    for copy in small[1:]:
        copy.wait()
    for j in range(n):
        own = slice(j * cols, (j + 1) * cols)
        gains[j, 0:1, :] = gain_one[...].astype(F32)[None, own]
        gains[j, 1:2, :] = gain_two[...].astype(F32)[None, own]
    token = lax.broadcasted_iota(jnp.int32, (tokens, LANES), 0)
    place = jnp.zeros((tokens, LANES), jnp.int32)
    for b in range(batches):
        place = jnp.where(token // steps == b, lengths[b] + token % steps, place)
        misc[2, b : b + 1, :] = jnp.full((1, LANES), lengths[b], jnp.int32).astype(F32)
    angle = place.astype(F32) * frequency
    sine = jnp.sin(angle)
    first = lax.broadcasted_iota(jnp.int32, (tokens, LANES), 1) < HEAD_DIM // 2
    misc[0] = jnp.cos(angle)
    misc[1] = jnp.where(first, -sine, sine)

    for copy in copies:
        copy.wait()
    found = rows[...].astype(F32).reshape(tokens * 8, width).astype(BF16)
    wide[...] = jnp.dot(one_hot, found, preferred_element_type=F32)
    square = jnp.sum(wide[...] * wide[...], axis=1, keepdims=True)
    spare = blocks.shape[2] - cols
    at = lax.broadcasted_iota(jnp.int32, (tokens, spare), 1)
    extra = jnp.zeros((tokens, spare), F32)
    for i, piece in enumerate(pieces_of(square, 3)):
        extra = jnp.where(at == i, piece, extra)
    extra = extra.astype(BF16)
    for j in range(n):
        blocks[j, :, :cols] = wide[:, j * cols : (j + 1) * cols].astype(BF16)
        blocks[j, :, cols:] = extra


def layer_kernel(
    n,
    blocks,
    gains,
    misc,
    bias_hbm,
    qkv_hbm,
    keys_hbm,
    values_hbm,
    out_hbm,
    gate_hbm,
    up_hbm,
    down_hbm,
    attended_ref,
    layer_ref,
    bias,
    w_qkv,
    keys,
    values,
    w_out,
    w_gate,
    w_up,
    w_down,
    rows_in,
    joint_out,
    joint_in,
    heads_all,
    own_heads,
    part_out,
    part_in,
    fresh,
    spread,
    attended_all,
    mid_all,
    wide,
    down_out,
    down_in,
    load_sem,
    send_sem,
    recv_sem,
):
    me = lax.axis_index("seq")
    tokens = blocks.shape[1]
    block_width = blocks.shape[2]
    batches, local_len = keys.shape[0], keys.shape[1]
    steps = tokens // batches
    cols, width = w_out.shape
    units = w_gate.shape[1]
    pairs = KV_HEADS // 2
    group_width = GROUP * HEAD_DIM
    scale = 1.0 / math.sqrt(HEAD_DIM)
    first_owner = n // 2 - KV_HEADS // 2
    is_owner = (me >= first_owner) & (me < first_owner + KV_HEADS)
    mine = jnp.clip(me - first_owner, 0, KV_HEADS - 1)
    side = me // (n // 2)
    turn = (me // 2) % 2

    loads = [
        pltpu.make_async_copy(a, b, load_sem.at[i])
        for i, (a, b) in enumerate(
            (
                (qkv_hbm, w_qkv),
                (bias_hbm, bias),
                (keys_hbm, keys),
                (values_hbm, values),
                (out_hbm, w_out),
                (gate_hbm, w_gate),
                (up_hbm, w_up),
                (down_hbm, w_down),
            )
        )
    ]
    barrier = pltpu.get_barrier_semaphore()

    @pl.loop(1, n)
    def _(d):
        pl.semaphore_signal(
            barrier, inc=1, device_id={"seq": lax.rem(me + d, n)}, device_id_type=MESH
        )

    for load in loads:
        load.start()

    unrolled = n & (n - 1) == 0 and n <= 32
    staged = unrolled and n // 4 <= 6 and cols % 16 == 0 and (4 * cols) % LANES == 0
    bits = n.bit_length() - 1
    flips = [(1 << k) * (1 - 2 * ((me // (1 << k)) % 2)) for k in range(bits)]

    def partner(d):
        return me + sum(flips[k] for k in range(bits) if d >> k & 1)

    def arrival_of(d):
        return 0 if d == 1 else 1 if d < 4 else 1 + d // 4

    def each_peer(act):
        if unrolled:
            for d in range(n - 1, 0, -1):
                act(partner(d))
        else:

            @pl.loop(1, n)
            def _(d):
                act(lax.rem(me + d, n))

    def copy_to(step, source, target, slot, peer, arrival=0):
        return pltpu.make_async_remote_copy(
            src_ref=source,
            dst_ref=target.at[slot],
            send_sem=send_sem.at[step],
            recv_sem=recv_sem.at[FIRST_RECEIVE[step] + arrival],
            device_id={"seq": peer},
            device_id_type=MESH,
        )

    def of_bytes(step, whole, arrival=0):
        return pltpu.make_async_remote_copy(
            src_ref=whole,
            dst_ref=whole,
            send_sem=send_sem.at[step],
            recv_sem=recv_sem.at[FIRST_RECEIVE[step] + arrival],
            device_id={"seq": lax.rem(me + 1, n)},
            device_id_type=MESH,
        )

    def landed(step, whole, arrival=0):
        of_bytes(step, whole, arrival).wait_recv()

    def departed(step, whole):
        of_bytes(step, whole).wait_send()

    def departed_to_owners(step, target):
        @pl.when(is_owner)
        def _():
            departed(step, target.at[pl.ds(0, KV_HEADS - 1)])

        @pl.when(jnp.logical_not(is_owner))
        def _():
            departed(step, target.at[pl.ds(0, KV_HEADS)])

    others = pl.ds(0, n - 1)

    def interleaved(s, count):
        picked = [wide[b * steps + s : b * steps + s + 1, :count] for b in range(batches)]
        return jnp.concatenate(picked, axis=0).astype(BF16)

    row = lax.broadcasted_iota(jnp.int32, (1, tokens, LANES), 1)
    upper = row < steps
    lane = lax.broadcasted_iota(jnp.int32, (tokens, LANES), 1)

    pl.semaphore_wait(barrier, n - 1)
    each_peer(lambda peer: copy_to(0, blocks.at[peer], rows_in, me, peer).start())
    rows_in[me] = blocks[me]
    for g in range(GROUP):
        at = lax.broadcasted_iota(jnp.int32, (LANES, LANES), 0)
        spread[:, g * LANES : (g + 1) * LANES] = jnp.where(
            (at >= g * 8) & (at < g * 8 + 3), 1.0, 0.0
        ).astype(BF16)
        spread[:, (GROUP + g) * LANES : (GROUP + g + 1) * LANES] = jnp.where(
            (at >= g * 8 + 3) & (at < g * 8 + 6), 1.0, 0.0
        ).astype(BF16)
    landed(0, rows_in.at[others])
    rows = rows_in[0].astype(F32)
    for j in range(1, n):
        rows += rows_in[j].astype(F32)
    stream = rows[:, :cols]
    square = jnp.sum(rows[:, cols : cols + 3], axis=1, keepdims=True)
    gain = gains[me]
    normed = (stream * lax.rsqrt(square / width + NORM_EPS) * gain[0:1]).astype(BF16)

    loads[0].wait()
    loads[1].wait()
    for i in range(pairs):
        c = side * i + (1 - side) * (pairs - 1 - i)
        q_part = jnp.dot(
            normed,
            w_qkv[:, pl.ds(pl.multiple_of(c * 2 * group_width, LANES), 2 * group_width)],
            preferred_element_type=F32,
        )
        k_part = jnp.dot(
            normed,
            w_qkv[:, pl.ds(pl.multiple_of((HEADS + 2 * c) * LANES, LANES), 2 * LANES)],
            preferred_element_type=F32,
        )
        v_part = jnp.dot(
            normed,
            w_qkv[:, pl.ds(pl.multiple_of((HEADS + KV_HEADS + 2 * c) * LANES, LANES), 2 * LANES)],
            preferred_element_type=F32,
        )
        for p in range(2):
            k = 2 * c + p
            owner = first_owner + k
            for g in range(GROUP):
                at = p * group_width + g * LANES
                joint_out[k, g] = q_part[:, at : at + LANES].astype(BF16)
            joint_out[k, GROUP] = k_part[:, p * LANES : (p + 1) * LANES].astype(BF16)
            joint_out[k, GROUP + 1] = v_part[:, p * LANES : (p + 1) * LANES].astype(BF16)

            @pl.when(owner != me)
            def _():
                copy_to(1, joint_out.at[k], joint_in, me, owner).start()

    departed(0, rows_in.at[others])

    @pl.when(is_owner)
    def _():
        joint_in[me] = joint_out[mine]
        landed(1, joint_in.at[others])
        joint = joint_in[0].astype(F32)
        for j in range(1, n):
            joint += joint_in[j].astype(F32)
        odd = mine % 2
        swap = jnp.full((tokens, LANES), odd, jnp.int32) == 1
        cos, sin = misc[0], misc[1]

        def biased(i, h):
            return (joint[i] + bias[pl.ds(h, 1), :]).astype(BF16).astype(F32)

        def turned(x):
            x = x * cos + pltpu.roll(x, HEAD_DIM // 2, 1) * sin
            return x.astype(BF16).astype(F32)

        for g in range(GROUP):
            x = turned(biased(g, mine * GROUP + g))
            x = jnp.where(swap, pltpu.roll(x, steps, 0), x)
            own_heads[g] = x
            heads_all[mine, g] = x.astype(BF16)
        each_peer(lambda peer: copy_to(2, heads_all.at[mine], heads_all, mine, peer, mine).start())
        own_heads[GROUP] = turned(biased(GROUP, HEADS + mine))
        own_heads[GROUP + 1] = biased(GROUP + 1, HEADS + KV_HEADS + mine)

        q = own_heads[:GROUP].reshape(GROUP * tokens, HEAD_DIM).astype(BF16)
        new_keys = own_heads[GROUP].astype(BF16)
        new_values = own_heads[GROUP + 1].astype(BF16)
        shape = (GROUP * tokens, tokens)
        at = lax.broadcasted_iota(jnp.int32, shape, 0) % tokens
        other = lax.broadcasted_iota(jnp.int32, shape, 1)
        prompt = (at // steps + odd) % 2
        seen = (other // steps == prompt) & (other % steps <= at % steps)
        score = lax.dot_general(q, new_keys, (((1,), (1,)), ((), ())), preferred_element_type=F32)
        score = jnp.where(seen, score * scale, MASKED)
        top = jnp.max(score, axis=1, keepdims=True)
        weight = jnp.where(seen, jnp.exp(score - top), 0.0)
        total = jnp.sum(weight, axis=1, keepdims=True)
        summed = jnp.dot(weight.astype(BF16), new_values, preferred_element_type=F32)
        wide_shape = (GROUP, tokens, LANES)
        fresh[0] = summed.reshape(wide_shape)
        fresh[1] = jnp.broadcast_to(top, (GROUP * tokens, LANES)).reshape(wide_shape)
        fresh[2] = jnp.broadcast_to(total, (GROUP * tokens, LANES)).reshape(wide_shape)

    departed_to_owners(1, joint_out)

    loads[2].wait()
    loads[3].wait()
    places = (
        me * local_len + lax.broadcasted_iota(jnp.int32, (1, local_len), 1)
    ).astype(F32)
    exponent = scale / math.log(2.0)
    order = [
        2 * side + turn,
        2 * side + 1 - turn,
        2 * (1 - side) + turn,
        2 * (1 - side) + 1 - turn,
    ]
    for near in range(2):
        for c in order[2 * near : 2 * near + 2]:
            for p in range(2):
                k = 2 * c + p

                @pl.when(first_owner + k != me)
                def _():
                    landed(2, heads_all.at[k], k)

        for c in order[2 * near : 2 * near + 2]:
            first = heads_all[2 * c].astype(F32)
            second = heads_all[2 * c + 1].astype(F32)
            pair_cols = pl.ds(pl.multiple_of(c * 2 * HEAD_DIM, LANES), 2 * HEAD_DIM)
            sums, tops, totals = [], [], []
            for b in range(batches):
                chosen = upper if b == 0 else ~upper
                q = jnp.concatenate(
                    [jnp.where(chosen, first, 0.0), jnp.where(chosen, 0.0, second)], axis=2
                )
                q = q.reshape(GROUP * tokens, 2 * HEAD_DIM).astype(BF16)
                scores = lax.dot_general(
                    q, keys[b, :, pair_cols], (((1,), (1,)), ((), ())), preferred_element_type=F32
                )
                scores = jnp.where(places < misc[2, b : b + 1, 0:1], scores, MASKED)
                top = jnp.max(scores, axis=1, keepdims=True)
                weight = jnp.exp2((scores - top) * exponent)
                total = jnp.sum(weight, axis=1, keepdims=True)
                summed = jnp.dot(
                    weight.astype(BF16), values[b, :, pair_cols], preferred_element_type=F32
                )
                sums.append(summed.reshape(GROUP, tokens, 2 * HEAD_DIM))
                wide_shape = (GROUP * tokens, LANES)
                tops.append(
                    jnp.broadcast_to(top * scale, wide_shape).reshape(GROUP, tokens, LANES)
                )
                totals.append(jnp.broadcast_to(total, wide_shape).reshape(GROUP, tokens, LANES))
            for p in range(2):
                k = 2 * c + p
                owner = first_owner + k
                low, high = (0, 1) if p == 0 else (1, 0)
                own = slice(p * HEAD_DIM, (p + 1) * HEAD_DIM)
                summed = jnp.where(upper, sums[low][:, :, own], sums[high][:, :, own])
                top = jnp.where(upper, tops[low], tops[high])
                total = jnp.where(upper, totals[low], totals[high])
                stats = jnp.zeros((tokens, LANES), F32)
                for i, piece in enumerate(pieces_of(top, 3) + pieces_of(total, 3)):
                    for g in range(GROUP):
                        stats = jnp.where(lane == g * 8 + i, piece[g], stats)
                part_out[k, :GROUP] = summed.astype(BF16)
                part_out[k, GROUP] = stats.astype(BF16)
        for c in order[2 * near : 2 * near + 2]:
            for p in range(2):
                k = 2 * c + p
                owner = first_owner + k

                @pl.when(owner != me)
                def _():
                    copy_to(3, part_out.at[k], part_in, me, owner).start()

    @pl.when(is_owner)
    def _():
        part_in[me] = part_out[mine]
        departed(2, joint_in.at[others, pl.ds(0, GROUP)])
        landed(3, part_in.at[others])
        stats = part_in[:, GROUP].astype(F32).reshape(n * tokens, LANES).astype(BF16)
        stats = jnp.dot(stats, spread[...], preferred_element_type=F32)
        swap = jnp.full((tokens, LANES), mine % 2, jnp.int32) == 1
        for g in range(GROUP):
            tops = stats[:, g * LANES : (g + 1) * LANES].reshape(n, tokens, LANES)
            totals = stats[:, (GROUP + g) * LANES : (GROUP + g + 1) * LANES]
            totals = totals.reshape(n, tokens, LANES)
            top = fresh[1, g]
            for j in range(n):
                top = jnp.maximum(top, tops[j])
            factor = jnp.exp(fresh[1, g] - top)
            total = fresh[2, g] * factor
            summed = fresh[0, g] * factor
            for j in range(n):
                factor = jnp.exp(tops[j] - top)
                total += totals[j] * factor
                summed += part_in[j, g].astype(F32) * factor
            x = summed / total
            x = jnp.where(swap, pltpu.roll(x, steps, 0), x)
            attended_all[mine, g] = x.astype(BF16)
        each_peer(lambda peer: copy_to(4, attended_all.at[mine], attended_all, mine, peer, mine).start())

    departed_to_owners(3, part_out)

    loads[4].wait()
    projected = jnp.zeros((tokens, cols), F32)
    for c in order:
        for p in range(2):
            k = 2 * c + p

            @pl.when(first_owner + k != me)
            def _():
                landed(4, attended_all.at[k], k)

        x = jnp.concatenate(
            [attended_all[2 * c + p, g] for p in range(2) for g in range(GROUP)], axis=1
        )
        at = pl.ds(pl.multiple_of(c * 2 * group_width, LANES), 2 * group_width)
        wide[:, at] = x.astype(F32)
        projected += lax.dot_general(
            x, w_out[:, at], (((1,), (1,)), ((), ())), preferred_element_type=F32
        )
    mid = stream + projected
    square = jnp.sum(mid * mid, axis=1, keepdims=True)
    spare = block_width - cols
    at = lax.broadcasted_iota(jnp.int32, (tokens, spare), 1)
    extra = jnp.zeros((tokens, spare), F32)
    for i, piece in enumerate(pieces_of(square, 3)):
        extra = jnp.where(at == i, piece, extra)
    mid_all[me, :, :cols] = (mid * gain[1:2]).astype(BF16)
    mid_all[me, :, cols:] = extra.astype(BF16)
    if staged:
        for d in range(n - 1, 0, -1):
            copy_to(5, mid_all.at[me], mid_all, me, partner(d), arrival_of(d)).start()
    else:
        each_peer(lambda peer: copy_to(5, mid_all.at[me], mid_all, me, peer).start())

    for s in range(steps):
        attended_ref[s] = interleaved(s, width)

    @pl.when(is_owner)
    def _():
        departed(4, joint_in.at[others, pl.ds(0, GROUP)])

    loads[5].wait()
    loads[6].wait()
    quad = 4
    gate = jnp.zeros((tokens, units), F32)
    upper_units = jnp.zeros((tokens, units), F32)
    tail = jnp.zeros((tokens, spare), F32)
    if staged:
        batches_of = [(0,), (1,), (2, 3)] + [
            tuple(range(q * quad, (q + 1) * quad)) for q in range(1, n // quad)
        ]
        for members in batches_of:
            if members[0]:
                start = partner(members[0]) // len(members) * len(members)
                landed(5, mid_all.at[pl.ds(start, len(members))], arrival_of(members[0]))
            for d in members:
                j = partner(d)
                x = mid_all[j]
                tail += x[:, cols:].astype(F32)
                x = x[:, :cols]
                at = pl.ds(pl.multiple_of(j * cols, 16), cols)
                gate += jnp.dot(x, w_gate[at, :], preferred_element_type=F32)
                upper_units += jnp.dot(x, w_up[at, :], preferred_element_type=F32)
    else:
        landed(5, mid_all.at[others])
        for j in range(n):
            x = mid_all[j].astype(F32)
            tail += x[:, cols:]
            wide[:, j * cols : (j + 1) * cols] = x[:, :cols]
        x = wide[...].astype(BF16)
        gate = jnp.dot(x, w_gate[...], preferred_element_type=F32)
        upper_units = jnp.dot(x, w_up[...], preferred_element_type=F32)
    square = jnp.sum(tail[:, :3], axis=1, keepdims=True)
    factor = lax.rsqrt(square / width + NORM_EPS)
    gate = gate * factor
    upper_units = upper_units * factor
    hidden = (gate / (1.0 + jnp.exp(-gate)) * upper_units).astype(BF16)
    loads[7].wait()

    if staged:
        for q in range(n // quad - 1, -1, -1):
            base = partner(q * quad) // quad * quad
            at = pl.ds(pl.multiple_of(base * cols, LANES), quad * cols)
            part = jnp.dot(hidden, w_down[:, at], preferred_element_type=F32)
            for i in range(quad):
                j = base + i
                down_out[j] = part[:, i * cols : (i + 1) * cols].astype(BF16)
                if q:
                    copy_to(6, down_out.at[j], down_in, me, j).start()
                else:

                    @pl.when(j != me)
                    def _():
                        copy_to(6, down_out.at[j], down_in, me, j).start()

    else:
        wide[...] = jnp.dot(hidden, w_down[...], preferred_element_type=F32)
        for j in range(n):
            down_out[j] = wide[:, j * cols : (j + 1) * cols].astype(BF16)
        each_peer(lambda peer: copy_to(6, down_out.at[peer], down_in, me, peer).start())
    down_in[me] = down_out[me]
    departed(5, mid_all.at[others])
    landed(6, down_in.at[others])
    summed = down_in[0].astype(F32)
    for j in range(1, n):
        summed += down_in[j].astype(F32)
    wide[:, :cols] = mid + summed
    for s in range(steps):
        layer_ref[s] = interleaved(s, cols)
    departed(6, down_in.at[others])


def finish_kernel(attended, layer, attended_out, layer_out, sem):
    copies = [
        pltpu.make_async_copy(attended, attended_out, sem.at[0]),
        pltpu.make_async_copy(layer, layer_out, sem.at[1]),
    ]
    for copy in copies:
        copy.start()
    for copy in copies:
        copy.wait()


def body(
    token_ids,
    lengths,
    embed_table,
    attn_gain,
    w_qkv,
    qkv_bias,
    cache_keys,
    cache_values,
    w_out,
    mlp_gain,
    w_gate,
    w_up,
    w_down,
):
    n = lax.axis_size("seq")
    steps, batches = token_ids.shape
    tokens = steps * batches
    width = embed_table.shape[1]
    cols = w_out.shape[1]
    block_width = -(-(cols + 3) // LANES) * LANES
    vmem = pl.BlockSpec(memory_space=pltpu.VMEM)
    hbm = pl.BlockSpec(memory_space=pltpu.HBM)

    def in_hbm(a):
        return pltpu.with_memory_space_constraint(a, pltpu.HBM)

    def in_vmem(a):
        return pltpu.with_memory_space_constraint(a, pltpu.VMEM)

    blocks, gains, misc = pl.pallas_call(
        functools.partial(gather_kernel, n),
        out_shape=(
            pltpu.VMEM((n, tokens, block_width), BF16),
            pltpu.VMEM((n, 8, cols), F32),
            pltpu.VMEM((3, tokens, LANES), F32),
        ),
        in_specs=[hbm] * 5,
        out_specs=(vmem, vmem, vmem),
        scratch_shapes=[
            pltpu.SMEM((batches, steps), jnp.int32),
            pltpu.SMEM((batches,), jnp.int32),
            pltpu.VMEM((width,), BF16),
            pltpu.VMEM((width,), BF16),
            pltpu.VMEM((tokens, 8, width), BF16),
            pltpu.VMEM((tokens, width), F32),
            pltpu.SemaphoreType.DMA((4,)),
            pltpu.SemaphoreType.DMA((tokens,)),
        ],
        compiler_params=pltpu.CompilerParams(vmem_limit_bytes=60 * 1024 * 1024),
    )(*(in_hbm(a) for a in (token_ids.T, lengths, attn_gain, mlp_gain, embed_table)))
    joint_heads = HEADS + 2 * KV_HEADS
    attended, layer_out = pl.pallas_call(
        functools.partial(layer_kernel, n),
        out_shape=(
            pltpu.VMEM((steps, batches, width), BF16),
            pltpu.VMEM((steps, batches, cols), BF16),
        ),
        in_specs=[vmem] * 3 + [hbm] * 8,
        out_specs=(vmem, vmem),
        scratch_shapes=[
            pltpu.VMEM((joint_heads, HEAD_DIM), F32),
        ]
        + [
            pltpu.VMEM(a.shape, a.dtype)
            for a in (w_qkv, cache_keys, cache_values, w_out.T, w_gate, w_up, w_down)
        ]
        + [
            pltpu.VMEM((n, tokens, block_width), BF16),
            pltpu.VMEM((KV_HEADS, LOCAL, tokens, LANES), BF16),
            pltpu.VMEM((n, LOCAL, tokens, LANES), BF16),
            pltpu.VMEM((KV_HEADS, GROUP, tokens, LANES), BF16),
            pltpu.VMEM((LOCAL, tokens, LANES), F32),
            pltpu.VMEM((KV_HEADS, GROUP + 1, tokens, LANES), BF16),
            pltpu.VMEM((n, GROUP + 1, tokens, LANES), BF16),
            pltpu.VMEM((3, GROUP, tokens, LANES), F32),
            pltpu.VMEM((LANES, 2 * GROUP * LANES), BF16),
            pltpu.VMEM((KV_HEADS, GROUP, tokens, LANES), BF16),
            pltpu.VMEM((n, tokens, block_width), BF16),
            pltpu.VMEM((tokens, width), F32),
            pltpu.VMEM((n, tokens, cols), BF16),
            pltpu.VMEM((n, tokens, cols), BF16),
            pltpu.SemaphoreType.DMA((8,)),
            pltpu.SemaphoreType.DMA((7,)),
            pltpu.SemaphoreType.DMA((RECEIVES,)),
        ],
        compiler_params=pltpu.CompilerParams(
            collective_id=0, has_side_effects=True, vmem_limit_bytes=57 * 1024 * 1024
        ),
    )(
        *(in_vmem(a) for a in (blocks, gains, misc)),
        *(
            in_hbm(a)
            for a in (
                qkv_bias.reshape(joint_heads, HEAD_DIM),
                w_qkv,
                cache_keys,
                cache_values,
                w_out.T,
                w_gate,
                w_up,
                w_down,
            )
        ),
    )
    return pl.pallas_call(
        finish_kernel,
        out_shape=(
            jax.ShapeDtypeStruct(attended.shape, BF16),
            jax.ShapeDtypeStruct(layer_out.shape, BF16),
        ),
        in_specs=[vmem, vmem],
        out_specs=(hbm, hbm),
        scratch_shapes=[pltpu.SemaphoreType.DMA((2,))],
        compiler_params=pltpu.CompilerParams(vmem_limit_bytes=60 * 1024 * 1024),
    )(in_vmem(attended), in_vmem(layer_out))


def solution(mesh):
    return jax.shard_map(
        body,
        mesh=mesh,
        in_specs=(
            P(None, "parts"),
            P("parts"),
            P("seq", None),
            P(),
            P("seq", None),
            P(),
            P("parts", "seq", None),
            P("parts", "seq", None),
            P(None, "seq"),
            P(),
            P(None, "seq"),
            P(None, "seq"),
            P("seq", None),
        ),
        out_specs=(P(None, "parts", None), P(None, "parts", "seq")),
        check_vma=False,
    )
```

```python
import functools
import math

import jax
import jax.numpy as jnp
import numpy as np
from jax import lax
from jax.experimental import pallas as pl
from jax.experimental.pallas import tpu as pltpu
from jax.sharding import PartitionSpec as P

HEADS = 40
KV_HEADS = 8
HEAD_DIM = 128
GROUP = HEADS // KV_HEADS
LOCAL = GROUP + 2
LANES = 128

NORM_EPS = 1e-06
ROPE_BASE = 1000000.0
MASKED = -1e30
F32 = jnp.float32
BF16 = jnp.bfloat16
MESH = pl.DeviceIdType.MESH

PAIRS = KV_HEADS // 2
FIRST_RECEIVE = (0, 1, 2, 2 + PAIRS, 3 + PAIRS, 3 + 2 * PAIRS, 8 + 2 * PAIRS)
RECEIVES = 9 + 2 * PAIRS


def pieces_of(value, count):
    out = []
    for _ in range(count):
        piece = value.astype(BF16).astype(F32)
        out.append(piece)
        value = value - piece
    return out


def gather_kernel(
    n,
    ids_hbm,
    lengths_hbm,
    gain_one_hbm,
    gain_two_hbm,
    table,
    blocks,
    gains,
    misc,
    ids,
    lengths,
    gain_one,
    gain_two,
    rows,
    wide,
    sem,
    row_sem,
):
    me = lax.axis_index("seq")
    small = [
        pltpu.make_async_copy(a, b, sem.at[i])
        for i, (a, b) in enumerate(
            (
                (ids_hbm, ids),
                (lengths_hbm, lengths),
                (gain_one_hbm, gain_one),
                (gain_two_hbm, gain_two),
            )
        )
    ]
    for copy in small:
        copy.start()
    first = lax.broadcasted_iota(jnp.int32, (1, LANES), 1)
    half = HEAD_DIM // 2
    frequency = jnp.zeros((1, LANES), F32)
    for i in range(half):
        value = float(np.float32(ROPE_BASE ** (-2.0 * i / HEAD_DIM)))
        frequency = jnp.where(first % half == i, value, frequency)
    batches, steps = ids.shape
    small[0].wait()
    tokens = batches * steps
    vocab_rows, width = table.shape
    cols = width // n
    row = lax.broadcasted_iota(jnp.int32, (tokens, tokens * 8), 0)
    lane = lax.broadcasted_iota(jnp.int32, (tokens, tokens * 8), 1)
    target = jnp.full((tokens, tokens * 8), -1, jnp.int32)
    copies = []
    for t in range(tokens):
        local = ids[t // steps, t % steps] - me * vocab_rows
        inside = (local >= 0) & (local < vocab_rows)
        local = jnp.clip(local, 0, vocab_rows - 1)
        base = local // 8
        copy = pltpu.make_async_copy(
            table.at[pl.ds(pl.multiple_of(base * 8, 8), 8), :], rows.at[t], row_sem.at[t]
        )
        copy.start()
        copies.append(copy)
        target = jnp.where(row == t, jnp.where(inside, t * 8 + local - base * 8, -1), target)
    one_hot = jnp.where(lane == target, 1.0, 0.0).astype(BF16)

    for copy in small[1:]:
        copy.wait()
    for j in range(n):
        own = slice(j * cols, (j + 1) * cols)
        gains[j, 0:1, :] = gain_one[...].astype(F32)[None, own]
        gains[j, 1:2, :] = gain_two[...].astype(F32)[None, own]
    token = lax.broadcasted_iota(jnp.int32, (tokens, LANES), 0)
    place = jnp.zeros((tokens, LANES), jnp.int32)
    for b in range(batches):
        place = jnp.where(token // steps == b, lengths[b] + token % steps, place)
        misc[2, b : b + 1, :] = jnp.full((1, LANES), lengths[b], jnp.int32).astype(F32)
    angle = place.astype(F32) * frequency
    sine = jnp.sin(angle)
    first = lax.broadcasted_iota(jnp.int32, (tokens, LANES), 1) < HEAD_DIM // 2
    misc[0] = jnp.cos(angle)
    misc[1] = jnp.where(first, -sine, sine)

    for copy in copies:
        copy.wait()
    found = rows[...].astype(F32).reshape(tokens * 8, width).astype(BF16)
    wide[...] = jnp.dot(one_hot, found, preferred_element_type=F32)
    square = jnp.sum(wide[...] * wide[...], axis=1, keepdims=True)
    spare = blocks.shape[2] - cols
    at = lax.broadcasted_iota(jnp.int32, (tokens, spare), 1)
    extra = jnp.zeros((tokens, spare), F32)
    for i, piece in enumerate(pieces_of(square, 3)):
        extra = jnp.where(at == i, piece, extra)
    extra = extra.astype(BF16)
    for j in range(n):
        blocks[j, :, :cols] = wide[:, j * cols : (j + 1) * cols].astype(BF16)
        blocks[j, :, cols:] = extra


def layer_kernel(
    n,
    blocks,
    gains,
    misc,
    bias_hbm,
    qkv_hbm,
    keys_hbm,
    values_hbm,
    out_hbm,
    gate_hbm,
    up_hbm,
    down_hbm,
    attended_ref,
    layer_ref,
    bias,
    w_qkv,
    keys,
    values,
    w_out,
    w_gate,
    w_up,
    w_down,
    rows_in,
    joint_out,
    joint_in,
    heads_all,
    own_heads,
    part_out,
    part_in,
    fresh,
    spread,
    attended_all,
    mid_all,
    wide,
    down_out,
    down_in,
    held,
    load_sem,
    send_sem,
    recv_sem,
):
    me = lax.axis_index("seq")
    tokens = blocks.shape[1]
    block_width = blocks.shape[2]
    batches, local_len = keys.shape[0], keys.shape[1]
    steps = tokens // batches
    cols, width = w_out.shape
    units = w_gate.shape[1]
    group_width = GROUP * HEAD_DIM
    scale = 1.0 / math.sqrt(HEAD_DIM)
    first_owner = n // 2 - PAIRS
    is_owner = (me >= first_owner) & (me < first_owner + 2 * PAIRS) & (me % 2 == 1)
    mine = jnp.clip((me - first_owner) // 2, 0, PAIRS - 1)

    def owner_of(c):
        return first_owner + 2 * c + 1

    side = me // (n // 2)
    turn = (me // 2) % 2

    loads = [
        pltpu.make_async_copy(a, b, load_sem.at[i])
        for i, (a, b) in enumerate(
            (
                (qkv_hbm, w_qkv),
                (bias_hbm, bias),
                (keys_hbm, keys),
                (values_hbm, values),
                (out_hbm, w_out),
                (gate_hbm, w_gate),
                (up_hbm, w_up),
                (down_hbm, w_down),
            )
        )
    ]
    barrier = pltpu.get_barrier_semaphore()

    @pl.loop(1, n)
    def _(d):
        pl.semaphore_signal(
            barrier, inc=1, device_id={"seq": lax.rem(me + d, n)}, device_id_type=MESH
        )

    for load in loads:
        load.start()

    unrolled = n & (n - 1) == 0 and n <= 32
    staged = unrolled and n // 4 <= 4 and cols % 16 == 0 and (4 * cols) % LANES == 0
    bits = n.bit_length() - 1
    flips = [(1 << k) * (1 - 2 * ((me // (1 << k)) % 2)) for k in range(bits)]

    def partner(d):
        return me + sum(flips[k] for k in range(bits) if d >> k & 1)

    def arrival_of(d):
        return 0 if d == 1 else 1 if d < 4 else 1 + d // 4

    def each_peer(act):
        if unrolled:
            for d in range(n - 1, 0, -1):
                act(partner(d))
        else:

            @pl.loop(1, n)
            def _(d):
                act(lax.rem(me + d, n))

    def copy_to(step, source, target, slot, peer, arrival=0):
        return pltpu.make_async_remote_copy(
            src_ref=source,
            dst_ref=target.at[slot],
            send_sem=send_sem.at[step % 2],
            recv_sem=recv_sem.at[FIRST_RECEIVE[step] + arrival],
            device_id={"seq": peer},
            device_id_type=MESH,
        )

    def of_bytes(step, whole, arrival=0):
        return pltpu.make_async_remote_copy(
            src_ref=whole,
            dst_ref=whole,
            send_sem=send_sem.at[step % 2],
            recv_sem=recv_sem.at[FIRST_RECEIVE[step] + arrival],
            device_id={"seq": lax.rem(me + 1, n)},
            device_id_type=MESH,
        )

    def landed(step, whole, arrival=0):
        of_bytes(step, whole, arrival).wait_recv()

    def departed(step, whole):
        of_bytes(step, whole).wait_send()

    def departed_to_owners(step, target):
        @pl.when(is_owner)
        def _():
            departed(step, target.at[pl.ds(0, PAIRS - 1)])

        @pl.when(jnp.logical_not(is_owner))
        def _():
            departed(step, target.at[pl.ds(0, PAIRS)])

    others = pl.ds(0, n - 1)

    def interleaved(s, count):
        picked = [wide[b * steps + s : b * steps + s + 1, :count] for b in range(batches)]
        return jnp.concatenate(picked, axis=0).astype(BF16)

    row = lax.broadcasted_iota(jnp.int32, (1, tokens, LANES), 1)
    upper = row < steps
    lane = lax.broadcasted_iota(jnp.int32, (tokens, LANES), 1)

    pl.semaphore_wait(barrier, n - 1)
    each_peer(lambda peer: copy_to(0, blocks.at[peer], rows_in, me, peer).start())
    rows_in[me] = blocks[me]
    for g in range(GROUP):
        at = lax.broadcasted_iota(jnp.int32, (LANES, LANES), 0)
        spread[:, g * LANES : (g + 1) * LANES] = jnp.where(
            (at >= g * 8) & (at < g * 8 + 3), 1.0, 0.0
        ).astype(BF16)
        spread[:, (GROUP + g) * LANES : (GROUP + g + 1) * LANES] = jnp.where(
            (at >= g * 8 + 3) & (at < g * 8 + 6), 1.0, 0.0
        ).astype(BF16)
    landed(0, rows_in.at[others])
    rows = rows_in[0].astype(F32)
    for j in range(1, n):
        rows += rows_in[j].astype(F32)
    stream = rows[:, :cols]
    square = jnp.sum(rows[:, cols : cols + 3], axis=1, keepdims=True)
    gain = gains[me]
    normed = (stream * lax.rsqrt(square / width + NORM_EPS) * gain[0:1]).astype(BF16)

    loads[0].wait()
    loads[1].wait()
    def joint_part(at, count):
        return jnp.dot(
            normed,
            w_qkv[:, pl.ds(pl.multiple_of(at * LANES, LANES), count * LANES)],
            preferred_element_type=F32,
        ).astype(BF16)

    far_first = [side * i + (1 - side) * (PAIRS - 1 - i) for i in range(PAIRS)]
    parts = None
    for i in range(PAIRS + 1):
        ready = parts
        if i < PAIRS:
            c = far_first[i]
            parts = (
                joint_part(2 * GROUP * c, 2 * GROUP),
                joint_part(HEADS + 2 * c, 2),
                joint_part(HEADS + KV_HEADS + 2 * c, 2),
            )
        if i:
            c = far_first[i - 1]
            for part, count, to in zip(ready, (GROUP, 1, 1), (0, GROUP, GROUP + 1)):
                for p in range(2):
                    for g in range(count):
                        at = (p * count + g) * LANES
                        joint_out[c, p, to + g] = part[:, at : at + LANES]

            @pl.when(owner_of(c) != me)
            def _():
                copy_to(1, joint_out.at[c], joint_in, me, owner_of(c)).start()

    departed(0, rows_in.at[others])

    @pl.when(is_owner)
    def _():
        joint_in[me] = joint_out[mine]
        landed(1, joint_in.at[others])
        cos, sin = misc[0], misc[1]

        def biased(p, i, h):
            joint = joint_in[0, p, i].astype(F32)
            for j in range(1, n):
                joint += joint_in[j, p, i].astype(F32)
            return (joint + bias[pl.ds(h, 1), :]).astype(BF16).astype(F32)

        def turned(x):
            x = x * cos + pltpu.roll(x, HEAD_DIM // 2, 1) * sin
            return x.astype(BF16).astype(F32)

        for p in range(2):
            k = 2 * mine + p
            for g in range(GROUP):
                x = turned(biased(p, g, k * GROUP + g))
                x = pltpu.roll(x, steps, 0) if p else x
                own_heads[p, g] = x
                heads_all[mine, p, g] = x.astype(BF16)
        each_peer(lambda peer: copy_to(2, heads_all.at[mine], heads_all, mine, peer, mine).start())

        for p in range(2):
            k = 2 * mine + p
            new_keys = turned(biased(p, GROUP, HEADS + k)).astype(BF16)
            new_values = biased(p, GROUP + 1, HEADS + KV_HEADS + k).astype(BF16)
            q = own_heads[p].reshape(GROUP * tokens, HEAD_DIM).astype(BF16)
            shape = (GROUP * tokens, tokens)
            at = lax.broadcasted_iota(jnp.int32, shape, 0) % tokens
            other = lax.broadcasted_iota(jnp.int32, shape, 1)
            prompt = (at // steps + p) % 2
            seen = (other // steps == prompt) & (other % steps <= at % steps)
            score = lax.dot_general(
                q, new_keys, (((1,), (1,)), ((), ())), preferred_element_type=F32
            )
            score = jnp.where(seen, score * scale, MASKED)
            top = jnp.max(score, axis=1, keepdims=True)
            weight = jnp.where(seen, jnp.exp(score - top), 0.0)
            total = jnp.sum(weight, axis=1, keepdims=True)
            summed = jnp.dot(weight.astype(BF16), new_values, preferred_element_type=F32)
            fresh[0, p] = summed.reshape(GROUP, tokens, LANES)
            for i, x in ((1, top), (2, total)):
                x = jnp.broadcast_to(x, (GROUP * tokens, LANES))
                fresh[i, p] = x.reshape(GROUP, tokens, LANES)

    departed_to_owners(1, joint_out)

    loads[2].wait()
    loads[3].wait()
    places = (
        me * local_len + lax.broadcasted_iota(jnp.int32, (1, local_len), 1)
    ).astype(F32)
    exponent = scale / math.log(2.0)
    near = [2 * side + turn, 2 * side + 1 - turn]
    far = [2 * (1 - side) + turn, 2 * (1 - side) + 1 - turn]
    order = [near[0], far[0], far[1], near[1]]
    def pair_cols(c):
        return pl.ds(pl.multiple_of(c * 2 * HEAD_DIM, LANES), 2 * HEAD_DIM)

    def scored(c, slot, b):
        chosen = upper if b == 0 else ~upper
        first = heads_all[c, 0].astype(F32)
        second = heads_all[c, 1].astype(F32)
        q = jnp.concatenate(
            [jnp.where(chosen, first, 0.0), jnp.where(chosen, 0.0, second)], axis=2
        )
        q = q.reshape(GROUP * tokens, 2 * HEAD_DIM).astype(BF16)
        scores = lax.dot_general(
            q, keys[b, :, pair_cols(c)], (((1,), (1,)), ((), ())), preferred_element_type=F32
        )
        scores = jnp.where(places < misc[2, b : b + 1, 0:1], scores, MASKED)
        held[slot, b] = scores
        return jnp.max(scores, axis=1, keepdims=True)

    def softened(slot, b, top):
        weight = jnp.exp2((held[slot, b] - top) * exponent)
        return weight.astype(BF16), jnp.sum(weight, axis=1, keepdims=True)

    def product(c, b, weight):
        summed = jnp.dot(weight, values[b, :, pair_cols(c)], preferred_element_type=F32)
        return summed.reshape(GROUP, tokens, 2 * HEAD_DIM)

    def packed(c, sums, tops, totals):
        def widened(x):
            return jnp.broadcast_to(x, (GROUP * tokens, LANES)).reshape(GROUP, tokens, LANES)

        tops = [widened(top * scale) for top in tops]
        totals = [widened(total) for total in totals]
        for p in range(2):
            low, high = (0, 1) if p == 0 else (1, 0)
            own = slice(p * HEAD_DIM, (p + 1) * HEAD_DIM)
            summed = jnp.where(upper, sums[low][:, :, own], sums[high][:, :, own])
            top = jnp.where(upper, tops[low], tops[high])
            total = jnp.where(upper, totals[low], totals[high])
            stats = jnp.zeros((tokens, LANES), F32)
            for i, piece in enumerate(pieces_of(top, 3) + pieces_of(total, 3)):
                for g in range(GROUP):
                    stats = jnp.where(lane == g * 8 + i, piece[g], stats)
            part_out[c, p, :GROUP] = summed.astype(BF16)
            part_out[c, p, GROUP] = stats.astype(BF16)

    found = {}
    for block in ((0,), (1, 2), (3, 4)):
        for r in block:
            if r < PAIRS:

                @pl.when(owner_of(order[r]) != me)
                def _():
                    landed(2, heads_all.at[order[r]], order[r])

        for r in block:
            before = r - 1
            if r < PAIRS:
                found[r] = [scored(order[r], r % 2, b) for b in range(batches)]
            if r:
                soft = [softened(before % 2, b, found[before][b]) for b in range(batches)]
                sums = [product(order[before], b, soft[b][0]) for b in range(batches)]
                packed(order[before], sums, found[before], [x[1] for x in soft])
        for r in block:
            if r:
                c = order[r - 1]

                @pl.when(owner_of(c) != me)
                def _():
                    copy_to(3, part_out.at[c], part_in, me, owner_of(c)).start()

    @pl.when(is_owner)
    def _():
        part_in[me] = part_out[mine]
        departed(2, joint_in.at[others, :, pl.ds(0, GROUP)])
        landed(3, part_in.at[others])
        for p in range(2):
            stats = part_in[:, p, GROUP].astype(F32).reshape(n * tokens, LANES).astype(BF16)
            stats = jnp.dot(stats, spread[...], preferred_element_type=F32)
            for g in range(GROUP):
                tops = stats[:, g * LANES : (g + 1) * LANES].reshape(n, tokens, LANES)
                totals = stats[:, (GROUP + g) * LANES : (GROUP + g + 1) * LANES]
                totals = totals.reshape(n, tokens, LANES)
                top = fresh[1, p, g]
                for j in range(n):
                    top = jnp.maximum(top, tops[j])
                factor = jnp.exp(fresh[1, p, g] - top)
                total = fresh[2, p, g] * factor
                summed = fresh[0, p, g] * factor
                for j in range(n):
                    factor = jnp.exp(tops[j] - top)
                    total += totals[j] * factor
                    summed += part_in[j, p, g].astype(F32) * factor
                x = summed / total
                x = pltpu.roll(x, steps, 0) if p else x
                attended_all[mine, p, g] = x.astype(BF16)
        each_peer(lambda peer: copy_to(4, attended_all.at[mine], attended_all, mine, peer, mine).start())

    departed_to_owners(3, part_out)

    loads[4].wait()
    projected = jnp.zeros((tokens, cols), F32)
    for c in near + far:

        @pl.when(owner_of(c) != me)
        def _():
            landed(4, attended_all.at[c], c)

        x = jnp.concatenate(
            [attended_all[c, p, g] for p in range(2) for g in range(GROUP)], axis=1
        )
        at = pl.ds(pl.multiple_of(c * 2 * group_width, LANES), 2 * group_width)
        wide[:, at] = x.astype(F32)
        projected += lax.dot_general(
            x, w_out[:, at], (((1,), (1,)), ((), ())), preferred_element_type=F32
        )
    mid = stream + projected
    square = jnp.sum(mid * mid, axis=1, keepdims=True)
    spare = block_width - cols
    at = lax.broadcasted_iota(jnp.int32, (tokens, spare), 1)
    extra = jnp.zeros((tokens, spare), F32)
    for i, piece in enumerate(pieces_of(square, 3)):
        extra = jnp.where(at == i, piece, extra)
    mid_all[me, :, :cols] = (mid * gain[1:2]).astype(BF16)
    mid_all[me, :, cols:] = extra.astype(BF16)
    if staged:
        for d in range(n - 1, 0, -1):
            copy_to(5, mid_all.at[me], mid_all, me, partner(d), arrival_of(d)).start()
    else:
        each_peer(lambda peer: copy_to(5, mid_all.at[me], mid_all, me, peer).start())

    for s in range(steps):
        attended_ref[s] = interleaved(s, width)

    @pl.when(is_owner)
    def _():
        departed(4, joint_in.at[others, :, pl.ds(0, GROUP)])

    loads[5].wait()
    loads[6].wait()
    quad = 4
    gate = jnp.zeros((tokens, units), F32)
    upper_units = jnp.zeros((tokens, units), F32)
    tail = jnp.zeros((tokens, spare), F32)
    if staged:
        batches_of = [(0,), (1,), (2, 3)] + [
            tuple(range(q * quad, (q + 1) * quad)) for q in range(1, n // quad)
        ]
        for members in batches_of:
            if members[0]:
                start = partner(members[0]) // len(members) * len(members)
                landed(5, mid_all.at[pl.ds(start, len(members))], arrival_of(members[0]))
            for d in members:
                j = partner(d)
                x = mid_all[j]
                tail += x[:, cols:].astype(F32)
                x = x[:, :cols]
                at = pl.ds(pl.multiple_of(j * cols, 16), cols)
                gate += jnp.dot(x, w_gate[at, :], preferred_element_type=F32)
                upper_units += jnp.dot(x, w_up[at, :], preferred_element_type=F32)
    else:
        landed(5, mid_all.at[others])
        for j in range(n):
            x = mid_all[j].astype(F32)
            tail += x[:, cols:]
            wide[:, j * cols : (j + 1) * cols] = x[:, :cols]
        x = wide[...].astype(BF16)
        gate = jnp.dot(x, w_gate[...], preferred_element_type=F32)
        upper_units = jnp.dot(x, w_up[...], preferred_element_type=F32)
    square = jnp.sum(tail[:, :3], axis=1, keepdims=True)
    factor = lax.rsqrt(square / width + NORM_EPS)
    gate = gate * factor
    upper_units = upper_units * factor
    hidden = (gate / (1.0 + jnp.exp(-gate)) * upper_units).astype(BF16)
    loads[7].wait()

    if staged:
        for q in range(n // quad - 1, -1, -1):
            base = partner(q * quad) // quad * quad
            at = pl.ds(pl.multiple_of(base * cols, LANES), quad * cols)
            part = jnp.dot(hidden, w_down[:, at], preferred_element_type=F32)
            for i in range(quad):
                j = base + i
                down_out[j] = part[:, i * cols : (i + 1) * cols].astype(BF16)
                if q:
                    copy_to(6, down_out.at[j], down_in, me, j).start()
                else:

                    @pl.when(j != me)
                    def _():
                        copy_to(6, down_out.at[j], down_in, me, j).start()

    else:
        wide[...] = jnp.dot(hidden, w_down[...], preferred_element_type=F32)
        for j in range(n):
            down_out[j] = wide[:, j * cols : (j + 1) * cols].astype(BF16)
        each_peer(lambda peer: copy_to(6, down_out.at[peer], down_in, me, peer).start())
    down_in[me] = down_out[me]
    departed(5, mid_all.at[others])
    landed(6, down_in.at[others])
    summed = down_in[0].astype(F32)
    for j in range(1, n):
        summed += down_in[j].astype(F32)
    wide[:, :cols] = mid + summed
    for s in range(steps):
        layer_ref[s] = interleaved(s, cols)
    departed(6, down_in.at[others])


def finish_kernel(attended, layer, attended_out, layer_out, sem):
    copies = [
        pltpu.make_async_copy(attended, attended_out, sem.at[0]),
        pltpu.make_async_copy(layer, layer_out, sem.at[1]),
    ]
    for copy in copies:
        copy.start()
    for copy in copies:
        copy.wait()


def body(
    token_ids,
    lengths,
    embed_table,
    attn_gain,
    w_qkv,
    qkv_bias,
    cache_keys,
    cache_values,
    w_out,
    mlp_gain,
    w_gate,
    w_up,
    w_down,
):
    n = lax.axis_size("seq")
    steps, batches = token_ids.shape
    tokens = steps * batches
    width = embed_table.shape[1]
    cols = w_out.shape[1]
    block_width = -(-(cols + 3) // LANES) * LANES
    vmem = pl.BlockSpec(memory_space=pltpu.VMEM)
    hbm = pl.BlockSpec(memory_space=pltpu.HBM)

    def in_hbm(a):
        return pltpu.with_memory_space_constraint(a, pltpu.HBM)

    def in_vmem(a):
        return pltpu.with_memory_space_constraint(a, pltpu.VMEM)

    blocks, gains, misc = pl.pallas_call(
        functools.partial(gather_kernel, n),
        out_shape=(
            pltpu.VMEM((n, tokens, block_width), BF16),
            pltpu.VMEM((n, 8, cols), F32),
            pltpu.VMEM((3, tokens, LANES), F32),
        ),
        in_specs=[hbm] * 5,
        out_specs=(vmem, vmem, vmem),
        scratch_shapes=[
            pltpu.SMEM((batches, steps), jnp.int32),
            pltpu.SMEM((batches,), jnp.int32),
            pltpu.VMEM((width,), BF16),
            pltpu.VMEM((width,), BF16),
            pltpu.VMEM((tokens, 8, width), BF16),
            pltpu.VMEM((tokens, width), F32),
            pltpu.SemaphoreType.DMA((4,)),
            pltpu.SemaphoreType.DMA((tokens,)),
        ],
        compiler_params=pltpu.CompilerParams(vmem_limit_bytes=60 * 1024 * 1024),
    )(*(in_hbm(a) for a in (token_ids.T, lengths, attn_gain, mlp_gain, embed_table)))
    joint_heads = HEADS + 2 * KV_HEADS
    attended, layer_out = pl.pallas_call(
        functools.partial(layer_kernel, n),
        out_shape=(
            pltpu.VMEM((steps, batches, width), BF16),
            pltpu.VMEM((steps, batches, cols), BF16),
        ),
        in_specs=[vmem] * 3 + [hbm] * 8,
        out_specs=(vmem, vmem),
        scratch_shapes=[
            pltpu.VMEM((joint_heads, HEAD_DIM), F32),
        ]
        + [
            pltpu.VMEM(a.shape, a.dtype)
            for a in (w_qkv, cache_keys, cache_values, w_out.T, w_gate, w_up, w_down)
        ]
        + [
            pltpu.VMEM((n, tokens, block_width), BF16),
            pltpu.VMEM((PAIRS, 2, LOCAL, tokens, LANES), BF16),
            pltpu.VMEM((n, 2, LOCAL, tokens, LANES), BF16),
            pltpu.VMEM((PAIRS, 2, GROUP, tokens, LANES), BF16),
            pltpu.VMEM((2, GROUP, tokens, LANES), F32),
            pltpu.VMEM((PAIRS, 2, GROUP + 1, tokens, LANES), BF16),
            pltpu.VMEM((n, 2, GROUP + 1, tokens, LANES), BF16),
            pltpu.VMEM((3, 2, GROUP, tokens, LANES), F32),
            pltpu.VMEM((LANES, 2 * GROUP * LANES), BF16),
            pltpu.VMEM((PAIRS, 2, GROUP, tokens, LANES), BF16),
            pltpu.VMEM((n, tokens, block_width), BF16),
            pltpu.VMEM((tokens, width), F32),
            pltpu.VMEM((n, tokens, cols), BF16),
            pltpu.VMEM((n, tokens, cols), BF16),
            pltpu.VMEM((2, batches, GROUP * tokens, cache_keys.shape[1]), F32),
            pltpu.SemaphoreType.DMA((8,)),
            pltpu.SemaphoreType.DMA((2,)),
            pltpu.SemaphoreType.DMA((RECEIVES,)),
        ],
        compiler_params=pltpu.CompilerParams(
            collective_id=0, has_side_effects=True, vmem_limit_bytes=62 * 1024 * 1024
        ),
    )(
        *(in_vmem(a) for a in (blocks, gains, misc)),
        *(
            in_hbm(a)
            for a in (
                qkv_bias.reshape(joint_heads, HEAD_DIM),
                w_qkv,
                cache_keys,
                cache_values,
                w_out.T,
                w_gate,
                w_up,
                w_down,
            )
        ),
    )
    return pl.pallas_call(
        finish_kernel,
        out_shape=(
            jax.ShapeDtypeStruct(attended.shape, BF16),
            jax.ShapeDtypeStruct(layer_out.shape, BF16),
        ),
        in_specs=[vmem, vmem],
        out_specs=(hbm, hbm),
        scratch_shapes=[pltpu.SemaphoreType.DMA((2,))],
        compiler_params=pltpu.CompilerParams(vmem_limit_bytes=60 * 1024 * 1024),
    )(in_vmem(attended), in_vmem(layer_out))


def solution(mesh):
    return jax.shard_map(
        body,
        mesh=mesh,
        in_specs=(
            P(None, "parts"),
            P("parts"),
            P("seq", None),
            P(),
            P("seq", None),
            P(),
            P("parts", "seq", None),
            P("parts", "seq", None),
            P(None, "seq"),
            P(),
            P(None, "seq"),
            P(None, "seq"),
            P("seq", None),
        ),
        out_specs=(P(None, "parts", None), P(None, "parts", "seq")),
        check_vma=False,
    )
```

```python
import functools
import math

import jax
import jax.numpy as jnp
import numpy as np
from jax import lax
from jax.experimental import pallas as pl
from jax.experimental.pallas import tpu as pltpu
from jax.sharding import PartitionSpec as P

HEADS = 40
KV_HEADS = 8
HEAD_DIM = 128
GROUP = HEADS // KV_HEADS
LOCAL = GROUP + 2
LANES = 128

NORM_EPS = 1e-06
ROPE_BASE = 1000000.0
MASKED = -1e30
F32 = jnp.float32
BF16 = jnp.bfloat16
MESH = pl.DeviceIdType.MESH

PAIRS = KV_HEADS // 2
FIRST_RECEIVE = (0, 1, 2, 2 + PAIRS, 3 + PAIRS, 3 + 2 * PAIRS, 8 + 2 * PAIRS)
RECEIVES = 9 + 2 * PAIRS


def pieces_of(value, count):
    out = []
    for _ in range(count):
        piece = value.astype(BF16).astype(F32)
        out.append(piece)
        value = value - piece
    return out


def gather_kernel(
    n,
    ids_hbm,
    lengths_hbm,
    gain_one_hbm,
    gain_two_hbm,
    table,
    blocks,
    gains,
    misc,
    ids,
    lengths,
    gain_one,
    gain_two,
    rows,
    wide,
    sem,
    row_sem,
):
    me = lax.axis_index("seq")
    small = [
        pltpu.make_async_copy(a, b, sem.at[i])
        for i, (a, b) in enumerate(
            (
                (ids_hbm, ids),
                (lengths_hbm, lengths),
                (gain_one_hbm, gain_one),
                (gain_two_hbm, gain_two),
            )
        )
    ]
    for copy in small:
        copy.start()
    first = lax.broadcasted_iota(jnp.int32, (1, LANES), 1)
    half = HEAD_DIM // 2
    frequency = jnp.zeros((1, LANES), F32)
    for i in range(half):
        value = float(np.float32(ROPE_BASE ** (-2.0 * i / HEAD_DIM)))
        frequency = jnp.where(first % half == i, value, frequency)
    batches, steps = ids.shape
    small[0].wait()
    tokens = batches * steps
    vocab_rows, width = table.shape
    cols = width // n
    row = lax.broadcasted_iota(jnp.int32, (tokens, tokens * 8), 0)
    lane = lax.broadcasted_iota(jnp.int32, (tokens, tokens * 8), 1)
    target = jnp.full((tokens, tokens * 8), -1, jnp.int32)
    for t in range(tokens):
        local = ids[t // steps, t % steps] - me * vocab_rows
        inside = (local >= 0) & (local < vocab_rows)
        local = jnp.clip(local, 0, vocab_rows - 1)
        base = local // 8
        copy = pltpu.make_async_copy(
            table.at[pl.ds(pl.multiple_of(base * 8, 8), 8), :], rows.at[t], row_sem
        )
        copy.start()
        target = jnp.where(row == t, jnp.where(inside, t * 8 + local - base * 8, -1), target)
    one_hot = jnp.where(lane == target, 1.0, 0.0).astype(BF16)

    for copy in small[1:]:
        copy.wait()
    for j in range(n):
        own = slice(j * cols, (j + 1) * cols)
        gains[j, 0:1, :] = gain_one[...].astype(F32)[None, own]
        gains[j, 1:2, :] = gain_two[...].astype(F32)[None, own]
    token = lax.broadcasted_iota(jnp.int32, (tokens, LANES), 0)
    place = jnp.zeros((tokens, LANES), jnp.int32)
    for b in range(batches):
        place = jnp.where(token // steps == b, lengths[b] + token % steps, place)
        misc[2, b : b + 1, :] = jnp.full((1, LANES), lengths[b], jnp.int32).astype(F32)
    angle = place.astype(F32) * frequency
    sine = jnp.sin(angle)
    first = lax.broadcasted_iota(jnp.int32, (tokens, LANES), 1) < HEAD_DIM // 2
    misc[0] = jnp.cos(angle)
    misc[1] = jnp.where(first, -sine, sine)

    pltpu.make_async_copy(rows, rows, row_sem).wait()
    found = rows[...].astype(F32).reshape(tokens * 8, width).astype(BF16)
    wide[...] = jnp.dot(one_hot, found, preferred_element_type=F32)
    square = jnp.sum(wide[...] * wide[...], axis=1, keepdims=True)
    spare = blocks.shape[2] - cols
    at = lax.broadcasted_iota(jnp.int32, (tokens, spare), 1)
    extra = jnp.zeros((tokens, spare), F32)
    for i, piece in enumerate(pieces_of(square, 3)):
        extra = jnp.where(at == i, piece, extra)
    extra = extra.astype(BF16)
    for j in range(n):
        blocks[j, :, :cols] = wide[:, j * cols : (j + 1) * cols].astype(BF16)
        blocks[j, :, cols:] = extra


def layer_kernel(
    n,
    blocks,
    gains,
    misc,
    bias_hbm,
    qkv_hbm,
    keys_hbm,
    values_hbm,
    out_hbm,
    gate_hbm,
    up_hbm,
    down_hbm,
    attended_ref,
    layer_ref,
    bias,
    w_qkv,
    keys,
    values,
    w_out,
    w_gate,
    w_up,
    w_down,
    rows_in,
    joint_out,
    joint_in,
    heads_all,
    own_heads,
    part_out,
    part_in,
    fresh,
    spread,
    attended_all,
    mid_all,
    wide,
    down_out,
    down_in,
    held,
    load_sem,
    send_sem,
    recv_sem,
):
    me = lax.axis_index("seq")
    tokens = blocks.shape[1]
    block_width = blocks.shape[2]
    batches, local_len = keys.shape[0], keys.shape[1]
    steps = tokens // batches
    cols, width = out_hbm.shape
    units = w_gate.shape[1]
    group_width = GROUP * HEAD_DIM
    scale = 1.0 / math.sqrt(HEAD_DIM)
    first_owner = n // 2 - PAIRS
    is_owner = (me >= first_owner) & (me < first_owner + 2 * PAIRS) & (me % 2 == 1)
    mine = jnp.clip((me - first_owner) // 2, 0, PAIRS - 1)

    def owner_of(c):
        return first_owner + 2 * c + 1

    side = me // (n // 2)
    turn = (me // 2) % 2

    loads = [
        pltpu.make_async_copy(a, b, load_sem.at[i])
        for i, (a, b) in enumerate(
            (
                (qkv_hbm, w_qkv.at[:, pl.ds(0, qkv_hbm.shape[1])]),
                (bias_hbm, bias),
                (keys_hbm, keys.at[:, :, pl.ds(0, keys_hbm.shape[2])]),
                (values_hbm, values.at[:, :, pl.ds(0, values_hbm.shape[2])]),
                (out_hbm, w_out.at[:, pl.ds(0, width)]),
                (gate_hbm, w_gate),
                (up_hbm, w_up),
                (down_hbm, w_down),
            )
        )
    ]
    barrier = pltpu.get_barrier_semaphore()

    unrolled = n & (n - 1) == 0 and n <= 32
    staged = unrolled and n // 4 <= 4 and cols % 16 == 0 and (4 * cols) % LANES == 0
    bits = n.bit_length() - 1
    flips = [(1 << k) * (1 - 2 * ((me // (1 << k)) % 2)) for k in range(bits)]

    def partner(d):
        return me + sum(flips[k] for k in range(bits) if d >> k & 1)

    def arrival_of(d):
        return 0 if d == 1 else 1 if d < 4 else 1 + d // 4

    def each_peer(act):
        if unrolled:
            for d in range(n - 1, 0, -1):
                act(partner(d))
        else:

            @pl.loop(1, n)
            def _(d):
                act(lax.rem(me + d, n))

    each_peer(
        lambda peer: pl.semaphore_signal(
            barrier, inc=1, device_id={"seq": peer}, device_id_type=MESH
        )
    )
    for load in loads:
        load.start()

    def copy_to(step, source, target, slot, peer, arrival=0):
        return pltpu.make_async_remote_copy(
            src_ref=source,
            dst_ref=target.at[slot],
            send_sem=send_sem.at[step % 2],
            recv_sem=recv_sem.at[FIRST_RECEIVE[step] + arrival],
            device_id={"seq": peer},
            device_id_type=MESH,
        )

    def of_bytes(step, whole, arrival=0):
        return pltpu.make_async_remote_copy(
            src_ref=whole,
            dst_ref=whole,
            send_sem=send_sem.at[step % 2],
            recv_sem=recv_sem.at[FIRST_RECEIVE[step] + arrival],
            device_id={"seq": lax.rem(me + 1, n)},
            device_id_type=MESH,
        )

    def landed(step, whole, arrival=0):
        of_bytes(step, whole, arrival).wait_recv()

    def departed(step, whole):
        of_bytes(step, whole).wait_send()

    def departed_to_owners(step, target):
        @pl.when(is_owner)
        def _():
            departed(step, target.at[pl.ds(0, PAIRS - 1)])

        @pl.when(jnp.logical_not(is_owner))
        def _():
            departed(step, target.at[pl.ds(0, PAIRS)])

    others = pl.ds(0, n - 1)

    def interleaved(s, count):
        picked = [wide[b * steps + s : b * steps + s + 1, :count] for b in range(batches)]
        return jnp.concatenate(picked, axis=0).astype(BF16)

    row = lax.broadcasted_iota(jnp.int32, (1, tokens, LANES), 1)
    upper = row < steps
    lane = lax.broadcasted_iota(jnp.int32, (tokens, LANES), 1)

    pl.semaphore_wait(barrier, n - 1)
    each_peer(lambda peer: copy_to(0, blocks.at[peer], rows_in, me, peer).start())
    rows_in[me] = blocks[me]
    for g in range(GROUP):
        at = lax.broadcasted_iota(jnp.int32, (LANES, LANES), 0)
        spread[:, g * LANES : (g + 1) * LANES] = jnp.where(
            (at >= g * 8) & (at < g * 8 + 3), 1.0, 0.0
        ).astype(BF16)
        spread[:, (GROUP + g) * LANES : (GROUP + g + 1) * LANES] = jnp.where(
            (at >= g * 8 + 3) & (at < g * 8 + 6), 1.0, 0.0
        ).astype(BF16)
    landed(0, rows_in.at[others])
    rows = rows_in[0].astype(F32)
    for j in range(1, n):
        rows += rows_in[j].astype(F32)
    stream = rows[:, :cols]
    square = jnp.sum(rows[:, cols : cols + 3], axis=1, keepdims=True)
    gain = gains[me]
    normed = (stream * lax.rsqrt(square / width + NORM_EPS) * gain[0:1]).astype(BF16)

    loads[0].wait()
    loads[1].wait()
    def joint_part(at, count):
        return jnp.dot(
            normed,
            w_qkv[:, pl.ds(pl.multiple_of(at * LANES, LANES), count * LANES)],
            preferred_element_type=F32,
        ).astype(BF16)

    far_first = [side * i + (1 - side) * (PAIRS - 1 - i) for i in range(PAIRS)]
    parts = None
    for i in range(PAIRS + 1):
        ready = parts
        if i < PAIRS:
            c = far_first[i]
            parts = (
                joint_part(2 * GROUP * c, 2 * GROUP),
                joint_part(HEADS + 2 * c, 2),
                joint_part(HEADS + KV_HEADS + 2 * c, 2),
            )
        if i:
            c = far_first[i - 1]
            for part, count, to in zip(ready, (GROUP, 1, 1), (0, GROUP, GROUP + 1)):
                for p in range(2):
                    for g in range(count):
                        at = (p * count + g) * LANES
                        joint_out[c, p, to + g] = part[:, at : at + LANES]

            @pl.when(owner_of(c) != me)
            def _():
                copy_to(1, joint_out.at[c], joint_in, me, owner_of(c)).start()

    departed(0, rows_in.at[others])

    @pl.when(is_owner)
    def _():
        joint_in[me] = joint_out[mine]
        landed(1, joint_in.at[others])
        cos, sin = misc[0], misc[1]

        def biased(p, i, h):
            joint = joint_in[0, p, i].astype(F32)
            for j in range(1, n):
                joint += joint_in[j, p, i].astype(F32)
            return (joint + bias[pl.ds(h, 1), :]).astype(BF16).astype(F32)

        def turned(x):
            x = x * cos + pltpu.roll(x, HEAD_DIM // 2, 1) * sin
            return x.astype(BF16).astype(F32)

        for p in range(2):
            k = 2 * mine + p
            for g in range(GROUP):
                x = turned(biased(p, g, k * GROUP + g))
                x = pltpu.roll(x, steps, 0) if p else x
                own_heads[p, g] = x
                heads_all[mine, p, g] = x.astype(BF16)
        each_peer(lambda peer: copy_to(2, heads_all.at[mine], heads_all, mine, peer, mine).start())

        for p in range(2):
            k = 2 * mine + p
            new_keys = turned(biased(p, GROUP, HEADS + k)).astype(BF16)
            new_values = biased(p, GROUP + 1, HEADS + KV_HEADS + k).astype(BF16)
            q = own_heads[p].reshape(GROUP * tokens, HEAD_DIM).astype(BF16)
            shape = (GROUP * tokens, tokens)
            at = lax.broadcasted_iota(jnp.int32, shape, 0) % tokens
            other = lax.broadcasted_iota(jnp.int32, shape, 1)
            prompt = (at // steps + p) % 2
            seen = (other // steps == prompt) & (other % steps <= at % steps)
            score = lax.dot_general(
                q, new_keys, (((1,), (1,)), ((), ())), preferred_element_type=F32
            )
            score = jnp.where(seen, score * scale, MASKED)
            top = jnp.max(score, axis=1, keepdims=True)
            weight = jnp.where(seen, jnp.exp(score - top), 0.0)
            total = jnp.sum(weight, axis=1, keepdims=True)
            summed = jnp.dot(weight.astype(BF16), new_values, preferred_element_type=F32)
            fresh[0, p] = summed.reshape(GROUP, tokens, LANES)
            for i, x in ((1, top), (2, total)):
                x = jnp.broadcast_to(x, (GROUP * tokens, LANES))
                fresh[i, p] = x.reshape(GROUP, tokens, LANES)

    departed_to_owners(1, joint_out)

    loads[2].wait()
    loads[3].wait()
    places = (
        me * local_len + lax.broadcasted_iota(jnp.int32, (1, local_len), 1)
    ).astype(F32)
    exponent = scale / math.log(2.0)
    near = [2 * side + turn, 2 * side + 1 - turn]
    far = [2 * (1 - side) + turn, 2 * (1 - side) + 1 - turn]
    order = [near[0], near[1], far[1], far[0]]
    def pair_cols(c):
        return pl.ds(pl.multiple_of(c * 2 * HEAD_DIM, LANES), 2 * HEAD_DIM)

    def scored(c, slot, b):
        chosen = upper if b == 0 else ~upper
        first = heads_all[c, 0].astype(F32)
        second = heads_all[c, 1].astype(F32)
        q = jnp.concatenate(
            [jnp.where(chosen, first, 0.0), jnp.where(chosen, 0.0, second)], axis=2
        )
        q = q.reshape(GROUP * tokens, 2 * HEAD_DIM).astype(BF16)
        scores = lax.dot_general(
            q, keys[b, :, pair_cols(c)], (((1,), (1,)), ((), ())), preferred_element_type=F32
        )
        scores = jnp.where(places < misc[2, b : b + 1, 0:1], scores, MASKED)
        held[slot, b] = scores
        return jnp.max(scores, axis=1, keepdims=True)

    def softened(slot, b, top):
        weight = jnp.exp2((held[slot, b] - top) * exponent)
        return weight.astype(BF16), jnp.sum(weight, axis=1, keepdims=True)

    def product(c, b, weight):
        summed = jnp.dot(weight, values[b, :, pair_cols(c)], preferred_element_type=F32)
        return summed.reshape(GROUP, tokens, 2 * HEAD_DIM)

    def packed(c, sums, tops, totals):
        def widened(x):
            return jnp.broadcast_to(x, (GROUP * tokens, LANES)).reshape(GROUP, tokens, LANES)

        tops = [widened(top * scale) for top in tops]
        totals = [widened(total) for total in totals]
        for p in range(2):
            low, high = (0, 1) if p == 0 else (1, 0)
            own = slice(p * HEAD_DIM, (p + 1) * HEAD_DIM)
            summed = jnp.where(upper, sums[low][:, :, own], sums[high][:, :, own])
            top = jnp.where(upper, tops[low], tops[high])
            total = jnp.where(upper, totals[low], totals[high])
            stats = jnp.zeros((tokens, LANES), F32)
            for i, piece in enumerate(pieces_of(top, 3) + pieces_of(total, 3)):
                for g in range(GROUP):
                    stats = jnp.where(lane == g * 8 + i, piece[g], stats)
            part_out[c, p, :GROUP] = summed.astype(BF16)
            part_out[c, p, GROUP] = stats.astype(BF16)

    found = {}
    for block in ((0, 1), (2,), (3, 4)):
        for r in block:
            if r < PAIRS:

                @pl.when(owner_of(order[r]) != me)
                def _():
                    landed(2, heads_all.at[order[r]], order[r])

        for r in block:
            before = r - 1
            if r < PAIRS:
                found[r] = [scored(order[r], r % 2, b) for b in range(batches)]
            if r:
                soft = [softened(before % 2, b, found[before][b]) for b in range(batches)]
                sums = [product(order[before], b, soft[b][0]) for b in range(batches)]
                packed(order[before], sums, found[before], [x[1] for x in soft])
        for r in block:
            if r:
                c = order[r - 1]

                @pl.when(owner_of(c) != me)
                def _():
                    copy_to(3, part_out.at[c], part_in, me, owner_of(c)).start()

    @pl.when(is_owner)
    def _():
        part_in[me] = part_out[mine]
        departed(2, joint_in.at[others, :, pl.ds(0, GROUP)])
        landed(3, part_in.at[others])
        for p in range(2):
            stats = part_in[:, p, GROUP].astype(F32).reshape(n * tokens, LANES).astype(BF16)
            stats = jnp.dot(stats, spread[...], preferred_element_type=F32)
            for g in range(GROUP):
                tops = stats[:, g * LANES : (g + 1) * LANES].reshape(n, tokens, LANES)
                totals = stats[:, (GROUP + g) * LANES : (GROUP + g + 1) * LANES]
                totals = totals.reshape(n, tokens, LANES)
                top = fresh[1, p, g]
                for j in range(n):
                    top = jnp.maximum(top, tops[j])
                factor = jnp.exp(fresh[1, p, g] - top)
                total = fresh[2, p, g] * factor
                summed = fresh[0, p, g] * factor
                for j in range(n):
                    factor = jnp.exp(tops[j] - top)
                    total += totals[j] * factor
                    summed += part_in[j, p, g].astype(F32) * factor
                x = summed / total
                x = pltpu.roll(x, steps, 0) if p else x
                attended_all[mine, p, g] = x.astype(BF16)
        each_peer(lambda peer: copy_to(4, attended_all.at[mine], attended_all, mine, peer, mine).start())

    departed_to_owners(3, part_out)

    loads[4].wait()
    projected = jnp.zeros((tokens, cols), F32)
    for c in near + far:

        @pl.when(owner_of(c) != me)
        def _():
            landed(4, attended_all.at[c], c)

        x = jnp.concatenate(
            [attended_all[c, p, g] for p in range(2) for g in range(GROUP)], axis=1
        )
        at = pl.ds(pl.multiple_of(c * 2 * group_width, LANES), 2 * group_width)
        wide[:, at] = x.astype(F32)
        projected += lax.dot_general(
            x, w_out[:, at], (((1,), (1,)), ((), ())), preferred_element_type=F32
        )
    mid = stream + projected
    square = jnp.sum(mid * mid, axis=1, keepdims=True)
    spare = block_width - cols
    at = lax.broadcasted_iota(jnp.int32, (tokens, spare), 1)
    extra = jnp.zeros((tokens, spare), F32)
    for i, piece in enumerate(pieces_of(square, 3)):
        extra = jnp.where(at == i, piece, extra)
    mid_all[me, :, :cols] = (mid * gain[1:2]).astype(BF16)
    mid_all[me, :, cols:] = extra.astype(BF16)
    if staged:
        for d in range(n - 1, 0, -1):
            copy_to(5, mid_all.at[me], mid_all, me, partner(d), arrival_of(d)).start()
    else:
        each_peer(lambda peer: copy_to(5, mid_all.at[me], mid_all, me, peer).start())

    for s in range(steps):
        attended_ref[s] = interleaved(s, width)

    @pl.when(is_owner)
    def _():
        departed(4, joint_in.at[others, :, pl.ds(0, GROUP)])

    loads[5].wait()
    loads[6].wait()
    quad = 4
    gate = jnp.zeros((tokens, units), F32)
    upper_units = jnp.zeros((tokens, units), F32)
    tail = jnp.zeros((tokens, spare), F32)
    if staged:
        batches_of = [(0,), (1,), (2, 3)] + [
            tuple(range(q * quad, (q + 1) * quad)) for q in range(1, n // quad)
        ]
        for members in batches_of:
            if members[0]:
                start = partner(members[0]) // len(members) * len(members)
                landed(5, mid_all.at[pl.ds(start, len(members))], arrival_of(members[0]))
            for d in members:
                j = partner(d)
                x = mid_all[j]
                tail += x[:, cols:].astype(F32)
                x = x[:, :cols]
                at = pl.ds(pl.multiple_of(j * cols, 16), cols)
                gate += jnp.dot(x, w_gate[at, :], preferred_element_type=F32)
                upper_units += jnp.dot(x, w_up[at, :], preferred_element_type=F32)
    else:
        landed(5, mid_all.at[others])
        for j in range(n):
            x = mid_all[j].astype(F32)
            tail += x[:, cols:]
            wide[:, j * cols : (j + 1) * cols] = x[:, :cols]
        x = wide[...].astype(BF16)
        gate = jnp.dot(x, w_gate[...], preferred_element_type=F32)
        upper_units = jnp.dot(x, w_up[...], preferred_element_type=F32)
    square = jnp.sum(tail[:, :3], axis=1, keepdims=True)
    factor = lax.rsqrt(square / width + NORM_EPS)
    gate = gate * factor
    upper_units = upper_units * factor
    hidden = (gate / (1.0 + jnp.exp(-gate)) * upper_units).astype(BF16)
    loads[7].wait()

    if staged:
        for q in range(n // quad - 1, -1, -1):
            base = partner(q * quad) // quad * quad
            at = pl.ds(pl.multiple_of(base * cols, LANES), quad * cols)
            part = jnp.dot(hidden, w_down[:, at], preferred_element_type=F32)
            for i in range(quad):
                j = base + i
                down_out[j] = part[:, i * cols : (i + 1) * cols].astype(BF16)
                if q:
                    copy_to(6, down_out.at[j], down_in, me, j).start()
                else:

                    @pl.when(j != me)
                    def _():
                        copy_to(6, down_out.at[j], down_in, me, j).start()

    else:
        wide[...] = jnp.dot(hidden, w_down[...], preferred_element_type=F32)
        for j in range(n):
            down_out[j] = wide[:, j * cols : (j + 1) * cols].astype(BF16)
        each_peer(lambda peer: copy_to(6, down_out.at[peer], down_in, me, peer).start())
    down_in[me] = down_out[me]
    departed(5, mid_all.at[others])
    landed(6, down_in.at[others])
    summed = down_in[0].astype(F32)
    for j in range(1, n):
        summed += down_in[j].astype(F32)
    wide[:, :cols] = mid + summed
    for s in range(steps):
        layer_ref[s] = interleaved(s, cols)
    departed(6, down_in.at[others])


def finish_kernel(attended, layer, attended_out, layer_out, sem):
    copies = [
        pltpu.make_async_copy(attended, attended_out, sem.at[0]),
        pltpu.make_async_copy(layer, layer_out, sem.at[1]),
    ]
    for copy in copies:
        copy.start()
    for copy in copies:
        copy.wait()


def body(
    token_ids,
    lengths,
    embed_table,
    attn_gain,
    w_qkv,
    qkv_bias,
    cache_keys,
    cache_values,
    w_out,
    mlp_gain,
    w_gate,
    w_up,
    w_down,
):
    n = lax.axis_size("seq")
    steps, batches = token_ids.shape
    tokens = steps * batches
    width = embed_table.shape[1]
    cols = w_out.shape[1]
    block_width = -(-(cols + 3) // LANES) * LANES
    vmem = pl.BlockSpec(memory_space=pltpu.VMEM)
    hbm = pl.BlockSpec(memory_space=pltpu.HBM)

    def in_hbm(a):
        return pltpu.with_memory_space_constraint(a, pltpu.HBM)

    def in_vmem(a):
        return pltpu.with_memory_space_constraint(a, pltpu.VMEM)

    blocks, gains, misc = pl.pallas_call(
        functools.partial(gather_kernel, n),
        out_shape=(
            pltpu.VMEM((n, tokens, block_width), BF16),
            pltpu.VMEM((n, 8, cols), F32),
            pltpu.VMEM((3, tokens, LANES), F32),
        ),
        in_specs=[hbm] * 5,
        out_specs=(vmem, vmem, vmem),
        scratch_shapes=[
            pltpu.SMEM((batches, steps), jnp.int32),
            pltpu.SMEM((batches,), jnp.int32),
            pltpu.VMEM((width,), BF16),
            pltpu.VMEM((width,), BF16),
            pltpu.VMEM((tokens, 8, width), BF16),
            pltpu.VMEM((tokens, width), F32),
            pltpu.SemaphoreType.DMA((4,)),
            pltpu.SemaphoreType.DMA,
        ],
        compiler_params=pltpu.CompilerParams(vmem_limit_bytes=60 * 1024 * 1024),
    )(*(in_hbm(a) for a in (token_ids.T, lengths, attn_gain, mlp_gain, embed_table)))
    joint_heads = HEADS + 2 * KV_HEADS
    attended, layer_out = pl.pallas_call(
        functools.partial(layer_kernel, n),
        out_shape=(
            pltpu.VMEM((steps, batches, width), BF16),
            pltpu.VMEM((steps, batches, cols), BF16),
        ),
        in_specs=[vmem] * 3 + [hbm] * 8,
        out_specs=(vmem, vmem),
        scratch_shapes=[
            pltpu.VMEM((joint_heads, HEAD_DIM), F32),
        ]
        + [
            pltpu.VMEM((*a.shape[:-1], a.shape[-1] + more), a.dtype)
            for a, more in (
                (w_qkv, 2 * LANES),
                (cache_keys, 2 * LANES),
                (cache_values, 2 * LANES),
                (w_out.T, 2 * LANES),
                (w_gate, 0),
                (w_up, 0),
                (w_down, 0),
            )
        ]
        + [
            pltpu.VMEM((n, tokens, block_width), BF16),
            pltpu.VMEM((PAIRS, 2, LOCAL, tokens, LANES), BF16),
            pltpu.VMEM((n, 2, LOCAL, tokens, LANES), BF16),
            pltpu.VMEM((PAIRS, 2, GROUP, tokens, LANES), BF16),
            pltpu.VMEM((2, GROUP, tokens, LANES), F32),
            pltpu.VMEM((PAIRS, 2, GROUP + 1, tokens, LANES), BF16),
            pltpu.VMEM((n, 2, GROUP + 1, tokens, LANES), BF16),
            pltpu.VMEM((3, 2, GROUP, tokens, LANES), F32),
            pltpu.VMEM((LANES, 2 * GROUP * LANES), BF16),
            pltpu.VMEM((PAIRS, 2, GROUP, tokens, LANES), BF16),
            pltpu.VMEM((n, tokens, block_width), BF16),
            pltpu.VMEM((tokens, width), F32),
            pltpu.VMEM((n, tokens, cols), BF16),
            pltpu.VMEM((n, tokens, cols), BF16),
            pltpu.VMEM((2, batches, GROUP * tokens, cache_keys.shape[1]), F32),
            pltpu.SemaphoreType.DMA((8,)),
            pltpu.SemaphoreType.DMA((2,)),
            pltpu.SemaphoreType.DMA((RECEIVES,)),
        ],
        compiler_params=pltpu.CompilerParams(
            collective_id=0, has_side_effects=True, vmem_limit_bytes=63 * 1024 * 1024
        ),
    )(
        *(in_vmem(a) for a in (blocks, gains, misc)),
        *(
            in_hbm(a)
            for a in (
                qkv_bias.reshape(joint_heads, HEAD_DIM),
                w_qkv,
                cache_keys,
                cache_values,
                w_out.T,
                w_gate,
                w_up,
                w_down,
            )
        ),
    )
    return pl.pallas_call(
        finish_kernel,
        out_shape=(
            jax.ShapeDtypeStruct(attended.shape, BF16),
            jax.ShapeDtypeStruct(layer_out.shape, BF16),
        ),
        in_specs=[vmem, vmem],
        out_specs=(hbm, hbm),
        scratch_shapes=[pltpu.SemaphoreType.DMA((2,))],
        compiler_params=pltpu.CompilerParams(vmem_limit_bytes=60 * 1024 * 1024),
    )(in_vmem(attended), in_vmem(layer_out))


def solution(mesh):
    return jax.shard_map(
        body,
        mesh=mesh,
        in_specs=(
            P(None, "parts"),
            P("parts"),
            P("seq", None),
            P(),
            P("seq", None),
            P(),
            P("parts", "seq", None),
            P("parts", "seq", None),
            P(None, "seq"),
            P(),
            P(None, "seq"),
            P(None, "seq"),
            P("seq", None),
        ),
        out_specs=(P(None, "parts", None), P(None, "parts", "seq")),
        check_vma=False,
    )
```
